512 devices in a mesh: dp: 64 (over y, z), aug: 8 (over x, core).
Axes of the slice: x: 4, y: 8, z: 8, core: 2. Of those that a mesh axis runs over, the one named last changes fastest.
Arguments:
- images: bfloat16 [8, 64, 197, 768], P('aug', 'dp'), may hold values from -6 to 6
- out_grads: bfloat16 [8, 64, 197, 768], P('aug', 'dp'), may hold values from -8 to 8
- up_weight_t: bfloat16 [3072, 768], P(('dp', 'aug')), may hold values from -0.21875 to 0.21875
- down_weight_t: bfloat16 [3072, 768], P(('dp', 'aug')), may hold values from -0.21875 to 0.21875
- left_up: bfloat16 [3072, 128], P(('dp', 'aug')), may hold values from -0.109375 to 0.109375
- right_up: bfloat16 [768, 128], replicated, may hold values from -0.21875 to 0.21875
- left_down: bfloat16 [768, 128], replicated, may hold values from -0.21875 to 0.21875
- right_down: bfloat16 [3072, 128], P(('dp', 'aug')), may hold values from -0.109375 to 0.109375
- noise: float32 [2, 128, 128], P(None, 'aug'), may hold values from -6 to 6
Outputs:
- update: float32 [2, 128, 128], P(None, 'aug')
- clip_scales: float32 [64], P('dp')
The draws below stay inside these ranges and needn't reach their ends.
All inputs are finite; a program needn't handle non-finite values.
Results may differ from the reference program's by a relative error of at most 0.0032.
Values may be sent and summed in bfloat16 or wider, within the bound.
No kernel may reach another device: no remote copies, remote signals or barrier semaphores. Data moves between devices by JAX's collectives and lax.ppermute only.
A program may use at most 64 MiB of HBM per device.

```python
import math
import jax
import jax.numpy as jnp
from jax import lax

D = 768
FF = 3072
RANK = 128
TOK = 197
IMG_DEV = 1
AUGS = 8
IMAGES = 64


def draw_out_grads(key, part):
    key_scale = jax.random.fold_in(key, 11)
    key_base = jax.random.fold_in(key, 12)
    shape = (AUGS, IMAGES, TOK, D)
    scales = jnp.exp(jax.random.uniform(key_scale, (IMAGES,), jnp.float32, math.log(0.1), 0.0))
    base = jnp.clip(jax.random.normal(key_base, shape, jnp.float32), -7.5, 7.5)
    return (base * scales[None, :, None, None]).astype(jnp.bfloat16)


def steps_of(stream_key, extent, split, low, top_value):
    loudness, own = 1.0, jax.random.fold_in(stream_key, 6)
    for axis_at, shards_of in split:
        heights = jnp.exp(jax.random.uniform(jax.random.fold_in(own, axis_at), (shards_of,), jnp.float32, low / len(split), top_value / len(split)))
        loudness = loudness * jnp.repeat(heights, extent[axis_at] // shards_of).reshape([-1 if axis == axis_at else 1 for axis in range(len(extent))])
    return loudness


def centred(key, extent, spread, reach, pieces=(), held_as=jnp.bfloat16):
    entries = spread * jax.random.normal(key, extent, jnp.float32)
    if pieces:
        entries = entries * steps_of(key, extent, pieces, -0.22, 0.18)
    return jnp.clip(entries, -reach, reach).astype(held_as)


def setup_inputs(seed: int = 0) -> dict:
    splits = jax.random.split(jax.random.key(seed), 10)
    images = centred(splits[0], (AUGS, IMAGES, TOK, D), 1.0, 6.0, ((0, 8), (1, 64)))
    out_grads = draw_out_grads(jax.random.fold_in(splits[9], 71), 0)
    up_weight_t = centred(splits[2], (FF, D), D ** -0.5, 0.21875, ((0, 512),))
    down_weight_t = centred(splits[3], (FF, D), D ** -0.5, 0.21875, ((0, 512),))
    left_up = centred(splits[4], (FF, RANK), FF ** -0.5, 0.109375, ((0, 512),))
    right_up = centred(splits[5], (D, RANK), D ** -0.5, 0.21875)
    left_down = centred(splits[6], (D, RANK), D ** -0.5, 0.21875)
    right_down = centred(splits[7], (FF, RANK), FF ** -0.5, 0.109375, ((0, 512),))
    noise = centred(splits[8], (2, RANK, RANK), 1.0, 6.0, ((1, 8),), jnp.float32)
    return {"images": images, "out_grads": out_grads, "up_weight_t": up_weight_t, "down_weight_t": down_weight_t, "left_up": left_up, "right_up": right_up, "left_down": left_down, "right_down": right_down, "noise": noise}


gelu_coef = 0.7978845608028654
clip_frac = 0.3
noise_mult = 0.05

def gelu_pair(hidden):
    inner = gelu_coef * (hidden + 0.044715 * hidden * hidden * hidden)
    tangent = jnp.tanh(inner)
    value = 0.5 * hidden * (1.0 + tangent)
    slope = 0.5 * (1.0 + tangent) + 0.5 * hidden * (1.0 - tangent * tangent) * gelu_coef * (1.0 + 3.0 * 0.044715 * hidden * hidden)
    return (value, slope)

def contract_last(left, right):
    return lax.dot_general(left, right, (((1,), (1,)), ((), ())), preferred_element_type=jnp.float32)

def block_terms(token_block, grad_block, up_weight_t, down_weight_t, left_up, right_up, left_down, right_down):
    count = token_block.shape[0]
    token_rows = token_block.reshape(-1, token_block.shape[-1])
    grad_rows = grad_block.reshape(-1, grad_block.shape[-1])
    hidden = contract_last(token_rows, up_weight_t)
    activation, slope = gelu_pair(hidden)
    activation = activation.astype(jnp.bfloat16)
    back = contract_last(grad_rows, down_weight_t)
    hidden_grad = (back * slope).astype(jnp.bfloat16)
    v_up = jnp.dot(hidden_grad, left_up, preferred_element_type=jnp.float32).astype(jnp.bfloat16)
    u_up = jnp.dot(token_rows, right_up, preferred_element_type=jnp.float32).astype(jnp.bfloat16)
    u_down = jnp.dot(activation, right_down, preferred_element_type=jnp.float32).astype(jnp.bfloat16)
    v_down = jnp.dot(grad_rows, left_down, preferred_element_type=jnp.float32).astype(jnp.bfloat16)
    shape = (count, TOK, RANK)
    first = jnp.einsum('itr,its->irs', v_up.reshape(shape).astype(jnp.float32), u_up.reshape(shape).astype(jnp.float32))
    second = jnp.einsum('itr,its->irs', v_down.reshape(shape).astype(jnp.float32), u_down.reshape(shape).astype(jnp.float32))
    return jnp.stack([first, second], axis=1)

def reference(images, out_grads, up_weight_t, down_weight_t, left_up, right_up, left_down, right_down, noise):
    blocks = IMAGES // IMG_DEV

    def per_aug(total, pair):
        aug_images, aug_grads = pair
        token_blocks = aug_images.reshape(blocks, IMG_DEV, TOK, D)
        grad_blocks = aug_grads.reshape(blocks, IMG_DEV, TOK, D)

        def one_block(inner):
            return block_terms(inner[0], inner[1], up_weight_t, down_weight_t, left_up, right_up, left_down, right_down)
        terms = lax.map(one_block, (token_blocks, grad_blocks))
        return (total + terms.reshape(IMAGES, 2, RANK, RANK), None)
    start = jnp.zeros((IMAGES, 2, RANK, RANK), jnp.float32)
    total, _ = lax.scan(per_aug, start, (images, out_grads))
    aug_mean = total / AUGS
    squares = lax.optimization_barrier(jnp.sum(aug_mean * aug_mean, axis=(1, 2, 3)))
    norms = jnp.sqrt(squares + 1e-06)
    clip_norm = clip_frac * RANK * math.sqrt(TOK / AUGS)
    clip_scales = jnp.minimum(1.0, clip_norm / norms)
    clipped_sum = lax.optimization_barrier(jnp.sum(clip_scales[:, None, None, None] * aug_mean, axis=0))
    update = (clipped_sum + noise_mult * clip_norm * noise) / jnp.sqrt(jnp.float32(IMAGES))
    return (update, clip_scales)
```

```python
import math

import jax
import jax.numpy as jnp
from jax import lax
from jax.sharding import Mesh
from jax.sharding import PartitionSpec as P

DP = ("dp_0", "dp_1")
AUG = ("x", "core")
bf16 = jnp.bfloat16
f32 = jnp.float32


gelu_coef = 0.7978845608028654
clip_frac = 0.3
noise_mult = 0.05


def copy_for_each(shard, axis):
    size = lax.axis_size(axis)
    return lax.all_to_all(
        jnp.broadcast_to(shard[None], (size, *shard.shape)), axis, 0, 0, tiled=True
    )


def of_everyone(shard, axis):
    return copy_for_each(shard, axis).astype(f32).sum(axis=0)


def gelu_pair(hidden):
    inner = gelu_coef * (hidden + 0.044715 * hidden * hidden * hidden)
    tangent = jnp.tanh(inner)
    value = 0.5 * hidden * (1.0 + tangent)
    slope = 0.5 * (1.0 + tangent) + 0.5 * hidden * (1.0 - tangent * tangent) * gelu_coef * (
        1.0 + 3.0 * 0.044715 * hidden * hidden
    )
    return (value, slope)


def contract(left, right, dims):
    return lax.dot_general(left, right, ((dims[0], dims[1]), ((), ())), preferred_element_type=f32)


def pack_weights(up, down, left, right):
    rows, width = up.shape
    flat = jnp.concatenate([left.reshape(1, width), right.reshape(1, width)], axis=1)
    both = jnp.concatenate([up, down], axis=1)
    fill = jnp.zeros((8 - rows - 1, 2 * width), bf16)
    return jnp.concatenate([both, flat, fill], axis=0)


def unpack_weights(gathered, rows, rank):
    senders, padded, twice = gathered.shape
    width = twice // 2
    picked = (rows + 1) * senders
    at = lax.broadcasted_iota(jnp.int32, (picked, senders * padded), 0)
    of = lax.broadcasted_iota(jnp.int32, (picked, senders * padded), 1)
    select = (of == (at % senders) * padded + at // senders).astype(bf16)
    both = contract(select, gathered.reshape(senders * padded, twice), ((1,), (0,))).astype(bf16)
    hidden_units = rows * senders
    up, down = both[:hidden_units, :width], both[:hidden_units, width:]
    flat = both[hidden_units:]
    left = jnp.concatenate([flat[:, r * rank : (r + 1) * rank] for r in range(rows)], axis=0)
    right = jnp.concatenate(
        [flat[:, width + r * rank : width + (r + 1) * rank] for r in range(rows)], axis=0
    )
    return up, down, left, right


def neighbour(array, shift):
    return lax.ppermute(array, "x", [(i, (i + shift) % 4) for i in range(4)])


def pad_rows(tokens):
    count, width = tokens.shape[-2:]
    return jnp.pad(tokens.reshape(count, width), ((0, -count % 8), (0, 0)))


def local(
    images, out_grads, up_weight_t, down_weight_t, left_up, right_up, left_down, right_down, noise
):
    tokens = images.shape[2]
    rank = right_up.shape[1]
    rows = up_weight_t.shape[0]
    packed = pack_weights(up_weight_t, down_weight_t, left_up, right_down)
    gathered = copy_for_each(packed, DP)
    mine = jnp.stack([pad_rows(images), pad_rows(out_grads)])
    below = neighbour(mine, 1)
    above = neighbour(mine, -1)
    far_tokens = neighbour(below[0], 1)
    far_grads = neighbour(above[1], -1)
    token_rows = jnp.concatenate([mine[0], below[0], above[0], far_tokens], axis=0)
    grad_rows = jnp.concatenate([mine[1], below[1], above[1], far_grads], axis=0)
    u_up = contract(token_rows, right_up, ((1,), (0,))).astype(bf16)
    v_down = contract(grad_rows, left_down, ((1,), (0,))).astype(bf16)
    partners = lax.ppermute(gathered, "core", [(0, 1), (1, 0)])
    v_up, u_down = 0.0, 0.0
    for part in (gathered, partners):
        up, down, left, right = unpack_weights(part, rows, rank)
        hidden = contract(token_rows, up, ((1,), (1,)))
        activation, slope = gelu_pair(hidden)
        back = contract(grad_rows, down, ((1,), (1,)))
        hidden_grad = (back * slope).astype(bf16)
        v_up += contract(hidden_grad, left, ((1,), (0,)))
        u_down += contract(activation.astype(bf16), right, ((1,), (0,)))
    first = contract(v_up.astype(bf16), u_up, ((0,), (0,)))
    second = contract(v_down, u_down.astype(bf16), ((0,), (0,)))
    terms = jnp.stack([first, second], axis=0).astype(bf16)
    all_augs = lax.axis_size(AUG)
    share_rows = rank // all_augs
    lower_row = lax.axis_index(AUG) * share_rows
    aug_mean = of_everyone(terms, AUG) / all_augs
    squares = jnp.sum(aug_mean * aug_mean)
    my_rows = lax.dynamic_slice_in_dim(aug_mean, lower_row, share_rows, 1)
    norm = jnp.sqrt(squares + 1e-06)
    clip_norm = clip_frac * rank * math.sqrt(tokens / all_augs)
    clip_scale = jnp.minimum(1.0, clip_norm / norm)
    summed_rows = of_everyone(of_everyone(clip_scale * my_rows, "dp_0"), "dp_1")
    all_images = lax.axis_size(DP)
    update = (summed_rows + noise_mult * clip_norm * noise) / jnp.sqrt(jnp.float32(all_images))
    return (update, clip_scale.reshape(1))


def solution(mesh):
    torus = Mesh(mesh.devices.reshape(8, 8, 4, 2), ("dp_0", "dp_1", "x", "core"))
    everyone = ("dp_0", "dp_1", "x", "core")
    placed = (
        P(AUG, DP, None, None),
        P(AUG, DP, None, None),
        P(everyone, None),
        P(everyone, None),
        P(everyone, None),
        P(),
        P(),
        P(everyone, None),
        P(None, AUG, None),
    )
    return jax.shard_map(
        local, mesh=torus, in_specs=placed, out_specs=(P(None, AUG, None), P(DP)), check_vma=False
    )
```

```python
import functools
import math

import jax
import jax.numpy as jnp
from jax import lax
from jax.experimental import pallas as pl
from jax.experimental.pallas import tpu as pltpu
from jax.sharding import Mesh
from jax.sharding import PartitionSpec as P


DP = ("dp_0", "dp_1")
AUG = ("x", "core")
bf16 = jnp.bfloat16
f32 = jnp.float32


gelu_coef = 0.7978845608028654
clip_frac = 0.3
noise_mult = 0.05
kernel_vmem = 24 * 2**20


def copy_for_each(shard, axis):
    size = lax.axis_size(axis)
    return lax.all_to_all(
        jnp.broadcast_to(shard[None], (size, *shard.shape)), axis, 0, 0, tiled=True
    )


def of_everyone(shard, axis):
    return copy_for_each(shard, axis).astype(f32).sum(axis=0)


def gelu_pair(hidden):
    square = hidden * hidden
    inner = hidden * (gelu_coef + (gelu_coef * 0.044715) * square)
    upper = 0.5 + 0.5 * jnp.tanh(inner)
    value = hidden * upper
    bend = 2.0 * gelu_coef + (6.0 * 0.044715 * gelu_coef) * square
    slope = upper + value * (1.0 - upper) * bend
    return (value, slope)


def contract(left, right, dims):
    return lax.dot_general(left, right, ((dims[0], dims[1]), ((), ())), preferred_element_type=f32)


def pack_weights(_, shards, fetches, results):
    up, down, left, right = shards
    (copies,) = results
    for fetch in fetches:
        fetch.wait()
    count, rows, lane = copies.shape[0], up.shape[0], left.shape[1]
    tiles = up.shape[1] // lane
    for wide, narrow, first in ((up, left, 0), (down, right, tiles)):
        for t in range(tiles):
            tile = jnp.concatenate(
                [
                    wide[:, t * lane : (t + 1) * lane].astype(f32),
                    narrow[t : t + 1, :].astype(f32),
                    jnp.zeros((8 - rows - 1, lane), f32),
                ],
                axis=0,
            ).astype(bf16)
            at = (first + t) * 8
            copies[:, at : at + 8, :] = jnp.broadcast_to(tile[None], (count, 8, lane))


def unpack_weights(gathered, senders, rank):
    height, twice = gathered.shape
    padded, width = height // senders, twice // 2
    rows = width // rank
    picked = (rows + 1) * senders
    at = lax.broadcasted_iota(jnp.int32, (picked, height), 0)
    of = lax.broadcasted_iota(jnp.int32, (picked, height), 1)
    select = (of == (at % senders) * padded + at // senders).astype(f32).astype(bf16)
    both = contract(select, gathered, ((1,), (0,))).astype(bf16)
    units = rows * senders
    up, down = both[:units, :width], both[:units, width:]
    flat = both[units:]
    left = jnp.concatenate([flat[:, r * rank : (r + 1) * rank] for r in range(rows)], axis=0)
    right = jnp.concatenate(
        [flat[:, width + r * rank : width + (r + 1) * rank] for r in range(rows)], axis=0
    )
    return up, down, left, right


def through_units(token_rows, grad_rows, weights):
    up, down, left, right = weights
    hidden = contract(token_rows, up, ((1,), (1,)))
    back = contract(grad_rows, down, ((1,), (1,)))
    activation, slope = gelu_pair(hidden)
    v_up = contract((back * slope).astype(bf16), left, ((1,), (0,)))
    u_down = contract(activation.astype(bf16), right, ((1,), (0,)))
    return v_up, u_down


def project(near, late, fetches, results):
    far, right_up, left_down = late
    u_up, v_down = results
    for fetch in fetches:
        fetch.wait()
    for k, group in enumerate((*near, far)):
        u_up[k] = contract(group[0], right_up[...], ((1,), (0,))).astype(bf16)
        v_down[k] = contract(group[1], left_down[...], ((1,), (0,))).astype(bf16)


def first_half(senders, rank, near, late, fetches, results):
    v_up, u_down = results
    unpacked = unpack_weights(near[0][...], senders, rank)
    for k, group in enumerate((*near[1:], late[0])):
        if k == len(near) - 1:
            fetches[0].wait()
        v_up[k], u_down[k] = through_units(group[0], group[1], unpacked)


def second_half(senders, rank, near, late, fetches, results):
    far, u_up, v_down, v_up, u_down = late
    (terms,) = results
    unpacked = unpack_weights(near[0][...], senders, rank)
    for fetch in fetches:
        fetch.wait()
    first, second = 0.0, 0.0
    for k, group in enumerate((*near[1:], far)):
        v_up_rest, u_down_rest = through_units(group[0], group[1], unpacked)
        v_up_all = (v_up[k] + v_up_rest).astype(bf16)
        u_down_all = (u_down[k] + u_down_rest).astype(bf16)
        first += contract(v_up_all, u_up[k], ((0,), (0,)))
        second += contract(v_down[k], u_down_all, ((0,), (0,)))
    both = jnp.stack([first, second]).astype(bf16)
    terms[...] = jnp.broadcast_to(both[None], terms.shape)


def held(arrays, space):
    return [pltpu.with_memory_space_constraint(a, space) for a in arrays]


def kernel(body, results, near, late=(), flops=0):
    def run(*refs):
        at, parts = 0, []
        for size in (len(near), len(late), len(results), len(late)):
            parts.append(refs[at : at + size])
            at += size
        near_refs, sources, result_refs, late_refs = parts
        fetches = [
            pltpu.make_async_copy(source, target, refs[at].at[i])
            for i, (source, target) in enumerate(zip(sources, late_refs))
        ]
        for fetch in fetches:
            fetch.start()
        body(near_refs, late_refs, fetches, result_refs)

    spec = pl.BlockSpec(memory_space=pltpu.VMEM)
    scratch = [pltpu.VMEM(a.shape, a.dtype) for a in late]
    call = pl.pallas_call(
        run,
        out_shape=tuple(pltpu.HBM(shape, dtype) for shape, dtype in results),
        in_specs=[spec] * len(near) + [pl.BlockSpec(memory_space=pltpu.HBM)] * len(late),
        out_specs=(spec,) * len(results),
        scratch_shapes=scratch + [pltpu.SemaphoreType.DMA((max(1, len(late)),))],
        compiler_params=pltpu.CompilerParams(vmem_limit_bytes=kernel_vmem),
        cost_estimate=pl.CostEstimate(flops=flops, bytes_accessed=10**6, transcendentals=0),
    )
    return call(*held(near, pltpu.VMEM), *held(late, pltpu.HBM))


def neighbour(array, shift):
    return lax.ppermute(array, "x", [(i, (i + shift) % 4) for i in range(4)])


def pad_rows(tokens):
    count, width = tokens.shape[-2:]
    return jnp.pad(tokens.reshape(count, width), ((0, -count % 8), (0, 0)))


def local(
    images, out_grads, up_weight_t, down_weight_t, left_up, right_up, left_down, right_down, noise
):
    tokens = images.shape[2]
    rank = right_up.shape[1]
    senders = lax.axis_size(DP)
    blocks = 2 * up_weight_t.shape[1] // rank
    shards = (up_weight_t, down_weight_t, left_up, right_down)
    (copies,) = kernel(pack_weights, [((senders, blocks * 8, rank), bf16)], (), shards)
    gathered = lax.all_to_all(copies, DP, 0, 0, tiled=True)
    gathered = gathered.reshape(senders, blocks, 8, rank).transpose(0, 2, 1, 3)
    gathered = gathered.reshape(senders * 8, blocks * rank)
    mine = jnp.stack([pad_rows(images), pad_rows(out_grads)])
    below = neighbour(mine, 1)
    above = neighbour(mine, -1)
    far = neighbour(mine, 2)
    partners = lax.ppermute(gathered, "core", [(0, 1), (1, 0)])
    groups = (mine, below, above)
    size = (len(groups) + 1, mine.shape[1], rank)
    kept = kernel(project, [(size, bf16)] * 2, groups, (far, right_up, left_down), flops=3 * 10**8)
    half = functools.partial(first_half, senders, rank)
    sums = kernel(half, [(size, f32)] * 2, (gathered, *groups), (far,), flops=2 * 10**9)
    all_augs = lax.axis_size(AUG)
    half = functools.partial(second_half, senders, rank)
    size = (all_augs, 2, rank, rank)
    (terms,) = kernel(
        half, [(size, bf16)], (partners, *groups), (far, *kept, *sums), flops=2 * 10**9
    )
    share_rows = rank // all_augs
    lower_row = lax.axis_index(AUG) * share_rows
    aug_mean = lax.all_to_all(terms, AUG, 0, 0, tiled=True).astype(f32).sum(axis=0) / all_augs
    squares = jnp.sum(aug_mean * aug_mean)
    my_rows = lax.dynamic_slice_in_dim(aug_mean, lower_row, share_rows, 1)
    norm = jnp.sqrt(squares + 1e-06)
    clip_norm = clip_frac * rank * math.sqrt(tokens / all_augs)
    clip_scale = jnp.minimum(1.0, clip_norm / norm)
    summed_rows = of_everyone(of_everyone(clip_scale * my_rows, "dp_0"), "dp_1")
    all_images = lax.axis_size(DP)
    update = (summed_rows + noise_mult * clip_norm * noise) / jnp.sqrt(jnp.float32(all_images))
    return (update, clip_scale.reshape(1))


def solution(mesh):
    torus = Mesh(mesh.devices.reshape(8, 8, 4, 2), ("dp_0", "dp_1", "x", "core"))
    everyone = ("dp_0", "dp_1", "x", "core")
    placed = (
        P(AUG, DP, None, None),
        P(AUG, DP, None, None),
        P(everyone, None),
        P(everyone, None),
        P(everyone, None),
        P(),
        P(),
        P(everyone, None),
        P(None, AUG, None),
    )
    return jax.shard_map(
        local, mesh=torus, in_specs=placed, out_specs=(P(None, AUG, None), P(DP)), check_vma=False
    )
```

```python
import functools
import math

import jax
import jax.numpy as jnp
from jax import lax
from jax.experimental import pallas as pl
from jax.experimental.pallas import tpu as pltpu
from jax.sharding import Mesh
from jax.sharding import PartitionSpec as P


DP = ("dp_0", "dp_1")
AUG = ("x", "core")
bf16 = jnp.bfloat16
f32 = jnp.float32


gelu_coef = 0.7978845608028654
clip_frac = 0.3
noise_mult = 0.05
kernel_vmem = 24 * 2**20


def copy_for_each(shard, axis):
    size = lax.axis_size(axis)
    return lax.all_to_all(
        jnp.broadcast_to(shard[None], (size, *shard.shape)), axis, 0, 0, tiled=True
    )


def of_everyone(shard, axis):
    return copy_for_each(shard, axis).astype(f32).sum(axis=0)


def gelu_pair(hidden):
    square = hidden * hidden
    inner = hidden * (gelu_coef + (gelu_coef * 0.044715) * square)
    upper = 0.5 + 0.5 * jnp.tanh(inner)
    value = hidden * upper
    bend = 2.0 * gelu_coef + (6.0 * 0.044715 * gelu_coef) * square
    slope = upper + value * (1.0 - upper) * bend
    return (value, slope)


def contract(left, right, dims):
    return lax.dot_general(left, right, ((dims[0], dims[1]), ((), ())), preferred_element_type=f32)


def pack_weights(_, shards, fetches, results):
    up, down, left, right = shards
    (copies,) = results
    for fetch in fetches:
        fetch.wait()
    count, rows, lane = copies.shape[0], up.shape[0], left.shape[1]
    tiles = up.shape[1] // lane
    for wide, narrow, first in ((up, left, 0), (down, right, tiles)):
        for t in range(tiles):
            tile = jnp.concatenate(
                [
                    wide[:, t * lane : (t + 1) * lane].astype(f32),
                    narrow[t : t + 1, :].astype(f32),
                    jnp.zeros((8 - rows - 1, lane), f32),
                ],
                axis=0,
            ).astype(bf16)
            at = (first + t) * 8
            copies[:, at : at + 8, :] = jnp.broadcast_to(tile[None], (count, 8, lane))


def unpack_weights(gathered, senders, rank):
    height, twice = gathered.shape
    padded, width = height // senders, twice // 2
    rows, block = width // rank, min(senders, 32)
    shape = ((rows + 1) * block, block * padded)
    at = lax.broadcasted_iota(jnp.int32, shape, 0)
    of = lax.broadcasted_iota(jnp.int32, shape, 1)
    select = (of == (at % block) * padded + at // block).astype(f32).astype(bf16)
    units = rows * block
    up, down, left, right = [], [], [], []
    for first in range(0, height, block * padded):
        piece = gathered[first : first + block * padded]
        both = contract(select, piece, ((1,), (0,))).astype(bf16)
        up.append(both[:units, :width])
        down.append(both[:units, width:])
        flat = both[units:]
        left += [flat[:, r * rank : (r + 1) * rank] for r in range(rows)]
        right += [flat[:, width + r * rank : width + (r + 1) * rank] for r in range(rows)]
    return tuple(jnp.concatenate(parts, axis=0) for parts in (up, down, left, right))


def through_units(token_rows, grad_rows, weights):
    up, down, left, right = weights
    hidden = contract(token_rows, up, ((1,), (1,)))
    back = contract(grad_rows, down, ((1,), (1,)))
    activation, slope = gelu_pair(hidden)
    v_up = contract((back * slope).astype(bf16), left, ((1,), (0,)))
    u_down = contract(activation.astype(bf16), right, ((1,), (0,)))
    return v_up, u_down


def first_half(senders, rank, near, late, fetches, results):
    right_up, left_down = late
    v_up, u_up, u_down, v_down = results
    unpacked = unpack_weights(near[0][...], senders, rank)
    for fetch in fetches:
        fetch.wait()
    for k, group in enumerate(near[1:]):
        v_up[k], u_down[k] = through_units(group[0], group[1], unpacked)
        u_up[k] = contract(group[0], right_up[...], ((1,), (0,))).astype(bf16)
        v_down[k] = contract(group[1], left_down[...], ((1,), (0,))).astype(bf16)


def second_half(senders, rank, near, late, fetches, results):
    v_up, u_up, u_down, v_down = late
    (terms,) = results
    unpacked = unpack_weights(near[0][...], senders, rank)
    for fetch in fetches:
        fetch.wait()
    first, second = 0.0, 0.0
    for k, group in enumerate(near[1:]):
        v_up_rest, u_down_rest = through_units(group[0], group[1], unpacked)
        v_up_all = (v_up[k] + v_up_rest).astype(bf16)
        u_down_all = (u_down[k] + u_down_rest).astype(bf16)
        first += contract(v_up_all, u_up[k], ((0,), (0,)))
        second += contract(v_down[k], u_down_all, ((0,), (0,)))
    both = jnp.stack([first, second]).astype(bf16)
    terms[...] = jnp.broadcast_to(both[None], terms.shape)


def held(arrays, space):
    return [pltpu.with_memory_space_constraint(a, space) for a in arrays]


def kernel(body, results, near, late=(), flops=0, space=pltpu.HBM):
    def run(*refs):
        at, parts = 0, []
        for size in (len(near), len(late), len(results), len(late)):
            parts.append(refs[at : at + size])
            at += size
        near_refs, sources, result_refs, late_refs = parts
        fetches = [
            pltpu.make_async_copy(source, target, refs[at].at[i])
            for i, (source, target) in enumerate(zip(sources, late_refs))
        ]
        for fetch in fetches:
            fetch.start()
        body(near_refs, late_refs, fetches, result_refs)

    spec = pl.BlockSpec(memory_space=pltpu.VMEM)
    scratch = [pltpu.VMEM(a.shape, a.dtype) for a in late]
    call = pl.pallas_call(
        run,
        out_shape=tuple(space(shape, dtype) for shape, dtype in results),
        in_specs=[spec] * len(near) + [pl.BlockSpec(memory_space=pltpu.HBM)] * len(late),
        out_specs=(spec,) * len(results),
        scratch_shapes=scratch + [pltpu.SemaphoreType.DMA((max(1, len(late)),))],
        compiler_params=pltpu.CompilerParams(vmem_limit_bytes=kernel_vmem),
        cost_estimate=pl.CostEstimate(flops=flops, bytes_accessed=10**6, transcendentals=0),
    )
    return call(*held(near, pltpu.VMEM), *held(late, pltpu.HBM))


def neighbour(array, shift):
    return lax.ppermute(array, "x", [(i, (i + shift) % 4) for i in range(4)])


def pad_rows(tokens):
    count, width = tokens.shape[-2:]
    return jnp.pad(tokens.reshape(count, width), ((0, -count % 8), (0, 0)))


def local(
    images, out_grads, up_weight_t, down_weight_t, left_up, right_up, left_down, right_down, noise
):
    tokens = images.shape[2]
    rank = right_up.shape[1]
    senders = lax.axis_size(DP)
    blocks = 2 * up_weight_t.shape[1] // rank
    shards = (up_weight_t, down_weight_t, left_up, right_down)
    size = (senders, blocks * 8, rank)
    (copies,) = kernel(pack_weights, [(size, bf16)], (), shards, space=jax.ShapeDtypeStruct)
    gathered = lax.all_to_all(copies, DP, 0, 0, tiled=True)
    gathered = gathered.reshape(senders, blocks, 8, rank).transpose(0, 2, 1, 3)
    gathered = gathered.reshape(senders * 8, blocks * rank)
    mine = jnp.stack([pad_rows(images), pad_rows(out_grads)])
    far, below, above = (neighbour(mine, shift) for shift in (2, 1, -1))
    partners = lax.ppermute(gathered, "core", [(0, 1), (1, 0)])
    groups = (mine, below, above, far)
    size = (len(groups), mine.shape[1], rank)
    half = functools.partial(first_half, senders, rank)
    sums = kernel(
        half,
        [(size, f32), (size, bf16)] * 2,
        (gathered, *groups),
        (right_up, left_down),
        flops=2 * 10**9,
    )
    all_augs = lax.axis_size(AUG)
    half = functools.partial(second_half, senders, rank)
    size = (all_augs, 2, rank, rank)
    (terms,) = kernel(
        half, [(size, bf16)], (partners, *groups), sums, flops=2 * 10**9
    )
    share_rows = rank // all_augs
    lower_row = lax.axis_index(AUG) * share_rows
    aug_mean = lax.all_to_all(terms, AUG, 0, 0, tiled=True).astype(f32).sum(axis=0) / all_augs
    squares = jnp.sum(aug_mean * aug_mean)
    my_rows = lax.dynamic_slice_in_dim(aug_mean, lower_row, share_rows, 1)
    norm = jnp.sqrt(squares + 1e-06)
    clip_norm = clip_frac * rank * math.sqrt(tokens / all_augs)
    clip_scale = jnp.minimum(1.0, clip_norm / norm)
    summed_rows = of_everyone(of_everyone(clip_scale * my_rows, "dp_0"), "dp_1")
    all_images = lax.axis_size(DP)
    update = (summed_rows + noise_mult * clip_norm * noise) / jnp.sqrt(jnp.float32(all_images))
    return (update, clip_scale.reshape(1))


def solution(mesh):
    torus = Mesh(mesh.devices.reshape(8, 8, 4, 2), ("dp_0", "dp_1", "x", "core"))
    everyone = ("dp_0", "dp_1", "x", "core")
    placed = (
        P(AUG, DP, None, None),
        P(AUG, DP, None, None),
        P(everyone, None),
        P(everyone, None),
        P(everyone, None),
        P(),
        P(),
        P(everyone, None),
        P(None, AUG, None),
    )
    return jax.shard_map(
        local, mesh=torus, in_specs=placed, out_specs=(P(None, AUG, None), P(DP)), check_vma=False
    )
```

```python
import functools
import math

import jax
import jax.numpy as jnp
from jax import lax
from jax.experimental import pallas as pl
from jax.experimental.pallas import tpu as pltpu
from jax.sharding import Mesh
from jax.sharding import PartitionSpec as P


DP = ("dp_0", "dp_1")
AUG = ("x", "core")
bf16 = jnp.bfloat16
f32 = jnp.float32


gelu_coef = 0.7978845608028654
clip_frac = 0.3
noise_mult = 0.05
kernel_vmem = 24 * 2**20
lane = 128


def copy_for_each(shard, axis):
    size = lax.axis_size(axis)
    return lax.all_to_all(
        jnp.broadcast_to(shard[None], (size, *shard.shape)), axis, 0, 0, tiled=True
    )


def of_everyone(shard, axis):
    return copy_for_each(shard, axis).astype(f32).sum(axis=0)


def gelu_pair(hidden):
    square = hidden * hidden
    inner = hidden * (gelu_coef + (gelu_coef * 0.044715) * square)
    upper = 0.5 + 0.5 * jnp.tanh(inner)
    value = hidden * upper
    bend = 2.0 * gelu_coef + (6.0 * 0.044715 * gelu_coef) * square
    slope = upper + value * (1.0 - upper) * bend
    return (value, slope)


def contract(left, right, dims):
    return lax.dot_general(left, right, ((dims[0], dims[1]), ((), ())), preferred_element_type=f32)


def pack_weights(_, shards, fetches, results):
    (copies,) = results
    count, height, _ = copies.shape
    for fetch in fetches:
        fetch.wait()
    columns = [
        shard[:, at : at + lane].astype(f32)
        for shard in shards
        for at in range(0, shard.shape[1], lane)
    ]
    spare = height - sum(column.shape[0] for column in columns)
    columns.append(jnp.zeros((spare, lane), f32))
    tall = jnp.concatenate(columns, axis=0).astype(bf16)
    copies[...] = jnp.broadcast_to(tall[None], (count, height, lane))


def unpack_weights(gathered, senders, rows, lane):
    height, wide = gathered.shape
    tile, block = height // senders, min(senders, 32)
    columns = wide // lane * tile // rows
    size = block * tile
    at = lax.broadcasted_iota(jnp.int32, (size, size), 0)
    of = lax.broadcasted_iota(jnp.int32, (size, size), 1)
    select = (of == (at % block) * tile + at // block).astype(f32).astype(bf16)
    parts = []
    for first in range(0, height, size):
        both = contract(select, gathered[first : first + size], ((1,), (0,))).astype(bf16)

        def cell(row, column):
            t, s = divmod(column * rows + row, tile)
            return both[s * block : (s + 1) * block, t * lane : (t + 1) * lane]

        for row in range(rows):
            parts.append([cell(row, column) for column in range(columns)])
    half = (columns - 2) // 2
    wides = [
        jnp.concatenate([jnp.concatenate(p[lo : lo + half], axis=1) for p in parts], axis=0)
        for lo in (0, half)
    ]
    narrows = [jnp.concatenate([p[c] for p in parts], axis=0) for c in (columns - 2, columns - 1)]
    return (*wides, *narrows)


def through_units(token_rows, grad_rows, weights):
    up, down, left, right = weights
    hidden = contract(token_rows, up, ((1,), (1,)))
    back = contract(grad_rows, down, ((1,), (1,)))
    activation, slope = gelu_pair(hidden)
    v_up = contract((back * slope).astype(bf16), left, ((1,), (0,)))
    u_down = contract(activation.astype(bf16), right, ((1,), (0,)))
    return v_up, u_down


def first_half(senders, rows, near, late, fetches, results):
    right_up, left_down = late
    v_up, u_up, u_down, v_down = results
    unpacked = unpack_weights(near[0][...], senders, rows, lane)
    for fetch in fetches:
        fetch.wait()
    for k, group in enumerate(near[1:]):
        v_up[k], u_down[k] = through_units(group[0], group[1], unpacked)
        u_up[k] = contract(group[0], right_up[...], ((1,), (0,))).astype(bf16)
        v_down[k] = contract(group[1], left_down[...], ((1,), (0,))).astype(bf16)


def second_half(senders, rows, near, late, fetches, results):
    v_up, u_up, u_down, v_down = late
    (terms,) = results
    unpacked = unpack_weights(near[0][...], senders, rows, lane)
    for fetch in fetches:
        fetch.wait()
    first, second = 0.0, 0.0
    for k, group in enumerate(near[1:]):
        v_up_rest, u_down_rest = through_units(group[0], group[1], unpacked)
        v_up_all = (v_up[k] + v_up_rest).astype(bf16)
        u_down_all = (u_down[k] + u_down_rest).astype(bf16)
        first += contract(v_up_all, u_up[k], ((0,), (0,)))
        second += contract(v_down[k], u_down_all, ((0,), (0,)))
    both = jnp.stack([first, second]).astype(bf16)
    terms[...] = jnp.broadcast_to(both[None], terms.shape)


def held(arrays, space):
    return [pltpu.with_memory_space_constraint(a, space) for a in arrays]


def kernel(body, results, near, late=(), flops=0):
    def run(*refs):
        at, parts = 0, []
        for size in (len(near), len(late), len(results), len(late)):
            parts.append(refs[at : at + size])
            at += size
        near_refs, sources, result_refs, late_refs = parts
        fetches = [
            pltpu.make_async_copy(source, target, refs[at].at[i])
            for i, (source, target) in enumerate(zip(sources, late_refs))
        ]
        for fetch in fetches:
            fetch.start()
        body(near_refs, late_refs, fetches, result_refs)

    spec = pl.BlockSpec(memory_space=pltpu.VMEM)
    scratch = [pltpu.VMEM(a.shape, a.dtype) for a in late]
    call = pl.pallas_call(
        run,
        out_shape=tuple(pltpu.HBM(shape, dtype) for shape, dtype in results),
        in_specs=[spec] * len(near) + [pl.BlockSpec(memory_space=pltpu.HBM)] * len(late),
        out_specs=(spec,) * len(results),
        scratch_shapes=scratch + [pltpu.SemaphoreType.DMA((max(1, len(late)),))],
        compiler_params=pltpu.CompilerParams(vmem_limit_bytes=kernel_vmem),
        cost_estimate=pl.CostEstimate(flops=flops, bytes_accessed=10**6, transcendentals=0),
    )
    return call(*held(near, pltpu.VMEM), *held(late, pltpu.HBM))


def neighbour(array, shift):
    return lax.ppermute(array, "x", [(i, (i + shift) % 4) for i in range(4)])


def pad_rows(tokens):
    count, width = tokens.shape[-2:]
    return jnp.pad(tokens.reshape(count, width), ((0, -count % 8), (0, 0)))


def local(
    images, out_grads, up_weight_t, down_weight_t, left_up, right_up, left_down, right_down, noise
):
    tokens = images.shape[2]
    rank = right_up.shape[1]
    senders = lax.axis_size(DP)
    shards = (up_weight_t, down_weight_t, left_up, right_down)
    rows = up_weight_t.shape[0]
    blocks = -(-rows * sum(shard.shape[1] for shard in shards) // (8 * lane))
    size = (senders, blocks * 8, lane)
    (copies,) = kernel(pack_weights, [(size, bf16)], (), shards)
    gathered = lax.all_to_all(copies, DP, 0, 0, tiled=True)
    gathered = gathered.reshape(senders, blocks, 8, lane).transpose(0, 2, 1, 3)
    gathered = gathered.reshape(senders * 8, blocks * lane)
    mine = jnp.stack([pad_rows(images), pad_rows(out_grads)])
    far, below, above = (neighbour(mine, shift) for shift in (2, 1, -1))
    partners = lax.ppermute(gathered, "core", [(0, 1), (1, 0)])
    groups = (mine, below, above, far)
    size = (len(groups), mine.shape[1], rank)
    half = functools.partial(first_half, senders, rows)
    sums = kernel(
        half,
        [(size, f32), (size, bf16)] * 2,
        (gathered, *groups),
        (right_up, left_down),
        flops=2 * 10**9,
    )
    all_augs = lax.axis_size(AUG)
    half = functools.partial(second_half, senders, rows)
    size = (all_augs, 2, rank, rank)
    (terms,) = kernel(
        half, [(size, bf16)], (partners, *groups), sums, flops=2 * 10**9
    )
    share_rows = rank // all_augs
    lower_row = lax.axis_index(AUG) * share_rows
    aug_mean = lax.all_to_all(terms, AUG, 0, 0, tiled=True).astype(f32).sum(axis=0) / all_augs
    squares = jnp.sum(aug_mean * aug_mean)
    my_rows = lax.dynamic_slice_in_dim(aug_mean, lower_row, share_rows, 1)
    norm = jnp.sqrt(squares + 1e-06)
    clip_norm = clip_frac * rank * math.sqrt(tokens / all_augs)
    clip_scale = jnp.minimum(1.0, clip_norm / norm)
    summed_rows = of_everyone(of_everyone(clip_scale * my_rows, "dp_0"), "dp_1")
    all_images = lax.axis_size(DP)
    update = (summed_rows + noise_mult * clip_norm * noise) / jnp.sqrt(jnp.float32(all_images))
    return (update, clip_scale.reshape(1))


def solution(mesh):
    torus = Mesh(mesh.devices.reshape(8, 8, 4, 2), ("dp_0", "dp_1", "x", "core"))
    everyone = ("dp_0", "dp_1", "x", "core")
    placed = (
        P(AUG, DP, None, None),
        P(AUG, DP, None, None),
        P(everyone, None),
        P(everyone, None),
        P(everyone, None),
        P(),
        P(),
        P(everyone, None),
        P(None, AUG, None),
    )
    return jax.shard_map(
        local, mesh=torus, in_specs=placed, out_specs=(P(None, AUG, None), P(DP)), check_vma=False
    )
```

```python
import functools
import math

import jax
import jax.numpy as jnp
from jax import lax
from jax.experimental import pallas as pl
from jax.experimental.pallas import tpu as pltpu
from jax.sharding import Mesh
from jax.sharding import PartitionSpec as P


DP = ("dp_0", "dp_1")
AUG = ("x", "core")
bf16 = jnp.bfloat16
f32 = jnp.float32


gelu_coef = 0.7978845608028654
clip_frac = 0.3
noise_mult = 0.05
kernel_vmem = 24 * 2**20
lane = 128


def copy_for_each(shard, axis):
    size = lax.axis_size(axis)
    return lax.all_to_all(
        jnp.broadcast_to(shard[None], (size, *shard.shape)), axis, 0, 0, tiled=True
    )


def of_everyone(shard, axis):
    return copy_for_each(shard, axis).astype(f32).sum(axis=0)


def gelu_pair(hidden):
    square = hidden * hidden
    inner = hidden * (gelu_coef + (gelu_coef * 0.044715) * square)
    upper = 0.5 + 0.5 * jnp.tanh(inner)
    value = hidden * upper
    bend = 2.0 * gelu_coef + (6.0 * 0.044715 * gelu_coef) * square
    slope = upper + value * (1.0 - upper) * bend
    return (value, slope)


def contract(left, right, dims):
    return lax.dot_general(left, right, ((dims[0], dims[1]), ((), ())), preferred_element_type=f32)


def pack_weights(_, shards, fetches, results):
    (copies,) = results
    count, height, _ = copies.shape
    for fetch in fetches:
        fetch.wait()
    columns = [
        shard[:, at : at + lane].astype(f32)
        for shard in shards
        for at in range(0, shard.shape[1], lane)
    ]
    spare = height - sum(column.shape[0] for column in columns)
    columns.append(jnp.zeros((spare, lane), f32))
    tall = jnp.concatenate(columns, axis=0).astype(bf16)
    copies[...] = jnp.broadcast_to(tall[None], (count, height, lane))


def unpack_weights(gathered, senders, rows, lane):
    height, wide = gathered.shape
    tile, block = height // senders, min(senders, 32)
    columns = wide // lane * tile // rows
    size = block * tile
    at = lax.broadcasted_iota(jnp.int32, (size, size), 0)
    of = lax.broadcasted_iota(jnp.int32, (size, size), 1)
    select = (of == (at % block) * tile + at // block).astype(f32).astype(bf16)
    parts = []
    for first in range(0, height, size):
        both = contract(select, gathered[first : first + size], ((1,), (0,))).astype(bf16)

        def cell(row, column):
            t, s = divmod(column * rows + row, tile)
            return both[s * block : (s + 1) * block, t * lane : (t + 1) * lane]

        for row in range(rows):
            parts.append([cell(row, column) for column in range(columns)])
    half = (columns - 2) // 2
    wides = [
        jnp.concatenate([jnp.concatenate(p[lo : lo + half], axis=1) for p in parts], axis=0)
        for lo in (0, half)
    ]
    narrows = [jnp.concatenate([p[c] for p in parts], axis=0) for c in (columns - 2, columns - 1)]
    return (*wides, *narrows)


def through_units(token_rows, grad_rows, weights):
    up, down, left, right = weights
    hidden = contract(token_rows, up, ((1,), (1,)))
    back = contract(grad_rows, down, ((1,), (1,)))
    activation, slope = gelu_pair(hidden)
    v_up = contract((back * slope).astype(bf16), left, ((1,), (0,)))
    u_down = contract(activation.astype(bf16), right, ((1,), (0,)))
    return v_up, u_down


def all_units(senders, rows, near, late, fetches, results):
    weights, *groups = near
    right_up, left_down, *others = late
    (terms,) = results
    unpacked = unpack_weights(weights[...], senders, rows, lane)
    for fetch in fetches[:2]:
        fetch.wait()
    first, second = 0.0, 0.0
    for k, group in enumerate((*groups, *others)):
        if k >= len(groups):
            fetches[2 + k - len(groups)].wait()
        token_rows, grad_rows = group[0], group[1]
        v_up, u_down = through_units(token_rows, grad_rows, unpacked)
        u_up = contract(token_rows, right_up[...], ((1,), (0,))).astype(bf16)
        v_down = contract(grad_rows, left_down[...], ((1,), (0,))).astype(bf16)
        first += contract(v_up.astype(bf16), u_up, ((0,), (0,)))
        second += contract(v_down, u_down.astype(bf16), ((0,), (0,)))
    both = jnp.stack([first, second]).astype(bf16)
    terms[...] = jnp.broadcast_to(both[None], terms.shape)


def held(arrays, space):
    return [pltpu.with_memory_space_constraint(a, space) for a in arrays]


def kernel(body, results, near, late=(), flops=0):
    def run(*refs):
        at, parts = 0, []
        for size in (len(near), len(late), len(results), len(late)):
            parts.append(refs[at : at + size])
            at += size
        near_refs, sources, result_refs, late_refs = parts
        fetches = [
            pltpu.make_async_copy(source, target, refs[at].at[i])
            for i, (source, target) in enumerate(zip(sources, late_refs))
        ]
        for fetch in fetches:
            fetch.start()
        body(near_refs, late_refs, fetches, result_refs)

    spec = pl.BlockSpec(memory_space=pltpu.VMEM)
    scratch = [pltpu.VMEM(a.shape, a.dtype) for a in late]
    call = pl.pallas_call(
        run,
        out_shape=tuple(pltpu.HBM(shape, dtype) for shape, dtype in results),
        in_specs=[spec] * len(near) + [pl.BlockSpec(memory_space=pltpu.HBM)] * len(late),
        out_specs=(spec,) * len(results),
        scratch_shapes=scratch + [pltpu.SemaphoreType.DMA((max(1, len(late)),))],
        compiler_params=pltpu.CompilerParams(vmem_limit_bytes=kernel_vmem),
        cost_estimate=pl.CostEstimate(flops=flops, bytes_accessed=10**6, transcendentals=0),
    )
    return call(*held(near, pltpu.VMEM), *held(late, pltpu.HBM))


def neighbour(array, shift):
    return lax.ppermute(array, "x", [(i, (i + shift) % 4) for i in range(4)])


def pad_rows(tokens):
    count, width = tokens.shape[-2:]
    return jnp.pad(tokens.reshape(count, width), ((0, -count % 8), (0, 0)))


def local(
    images, out_grads, up_weight_t, down_weight_t, left_up, right_up, left_down, right_down, noise
):
    tokens = images.shape[2]
    rank = right_up.shape[1]
    senders = lax.axis_size(DP)
    shards = (up_weight_t, down_weight_t, left_up, right_down)
    rows = up_weight_t.shape[0]
    blocks = -(-rows * sum(shard.shape[1] for shard in shards) // (8 * lane))
    size = (senders, blocks * 8, lane)
    (copies,) = kernel(pack_weights, [(size, bf16)], (), shards)
    gathered = lax.all_to_all(copies, DP, 0, 0, tiled=True)
    gathered = gathered.reshape(senders, blocks, 8, lane).transpose(0, 2, 1, 3)
    gathered = gathered.reshape(senders * 8, blocks * lane)
    mine = jnp.stack([pad_rows(images), pad_rows(out_grads)])
    far, below, above = (neighbour(mine, shift) for shift in (2, 1, -1))
    swapped = [lax.ppermute(g, "core", [(0, 1), (1, 0)]) for g in (mine, below, above, far)]
    all_augs = lax.axis_size(AUG)
    units = functools.partial(all_units, senders, rows)
    size = (all_augs, 2, rank, rank)
    near = (gathered, mine, below, above)
    late = (right_up, left_down, far, *swapped)
    (terms,) = kernel(units, [(size, bf16)], near, late, flops=4 * 10**9)
    share_rows = rank // all_augs
    lower_row = lax.axis_index(AUG) * share_rows
    aug_mean = lax.all_to_all(terms, AUG, 0, 0, tiled=True).astype(f32).sum(axis=0) / all_augs
    squares = jnp.sum(aug_mean * aug_mean)
    my_rows = lax.dynamic_slice_in_dim(aug_mean, lower_row, share_rows, 1)
    norm = jnp.sqrt(squares + 1e-06)
    clip_norm = clip_frac * rank * math.sqrt(tokens / all_augs)
    clip_scale = jnp.minimum(1.0, clip_norm / norm)
    summed_rows = of_everyone(of_everyone(clip_scale * my_rows, "dp_0"), "dp_1")
    all_images = lax.axis_size(DP)
    update = (summed_rows + noise_mult * clip_norm * noise) / jnp.sqrt(jnp.float32(all_images))
    return (update, clip_scale.reshape(1))


def solution(mesh):
    torus = Mesh(mesh.devices.reshape(8, 8, 4, 2), ("dp_0", "dp_1", "x", "core"))
    everyone = ("dp_0", "dp_1", "x", "core")
    placed = (
        P(AUG, DP, None, None),
        P(AUG, DP, None, None),
        P(everyone, None),
        P(everyone, None),
        P(everyone, None),
        P(),
        P(),
        P(everyone, None),
        P(None, AUG, None),
    )
    return jax.shard_map(
        local, mesh=torus, in_specs=placed, out_specs=(P(None, AUG, None), P(DP)), check_vma=False
    )
```

```python
import functools
import math

import jax
import jax.numpy as jnp
from jax import lax
from jax.experimental import pallas as pl
from jax.experimental.pallas import tpu as pltpu
from jax.sharding import Mesh
from jax.sharding import PartitionSpec as P


DP = ("dp_0", "dp_1")
AUG = ("x", "core")
bf16 = jnp.bfloat16
f32 = jnp.float32


gelu_coef = 0.7978845608028654
clip_frac = 0.3
noise_mult = 0.05
kernel_vmem = 24 * 2**20
lane = 128


def copy_for_each(shard, axis):
    size = lax.axis_size(axis)
    return lax.all_to_all(
        jnp.broadcast_to(shard[None], (size, *shard.shape)), axis, 0, 0, tiled=True
    )


def of_everyone(shard, axis):
    return copy_for_each(shard, axis).astype(f32).sum(axis=0)


def gelu_pair(hidden):
    square = hidden * hidden
    inner = hidden * (gelu_coef + (gelu_coef * 0.044715) * square)
    upper = 0.5 + 0.5 * jnp.tanh(inner)
    value = hidden * upper
    bend = 2.0 * gelu_coef + (6.0 * 0.044715 * gelu_coef) * square
    slope = upper + value * (1.0 - upper) * bend
    return (value, slope)


def contract(left, right, dims):
    return lax.dot_general(left, right, ((dims[0], dims[1]), ((), ())), preferred_element_type=f32)


def pack_weights(_, shards, fetches, results):
    (copies,) = results
    count, height, _ = copies.shape
    for fetch in fetches:
        fetch.wait()
    columns = [
        shard[:, at : at + lane].astype(f32)
        for shard in shards
        for at in range(0, shard.shape[1], lane)
    ]
    spare = height - sum(column.shape[0] for column in columns)
    columns.append(jnp.zeros((spare, lane), f32))
    tall = jnp.concatenate(columns, axis=0).astype(bf16)
    copies[...] = jnp.broadcast_to(tall[None], (count, height, lane))


def unpack_weights(gathered, senders, rows, lane):
    height, wide = gathered.shape
    tile, block = height // senders, min(senders, 32)
    columns = wide // lane * tile // rows
    size = block * tile
    at = lax.broadcasted_iota(jnp.int32, (size, size), 0)
    of = lax.broadcasted_iota(jnp.int32, (size, size), 1)
    select = (of == (at % block) * tile + at // block).astype(f32).astype(bf16)
    parts = []
    for first in range(0, height, size):
        both = contract(select, gathered[first : first + size], ((1,), (0,))).astype(bf16)

        def cell(row, column):
            t, s = divmod(column * rows + row, tile)
            return both[s * block : (s + 1) * block, t * lane : (t + 1) * lane]

        for row in range(rows):
            parts.append([cell(row, column) for column in range(columns)])
    half = (columns - 2) // 2
    wides = [
        jnp.concatenate([jnp.concatenate(p[lo : lo + half], axis=1) for p in parts], axis=0)
        for lo in (0, half)
    ]
    narrows = [jnp.concatenate([p[c] for p in parts], axis=0) for c in (columns - 2, columns - 1)]
    return (*wides, *narrows)


def through_units(token_rows, grad_rows, weights):
    up, down, left, right = weights
    hidden = contract(token_rows, up, ((1,), (1,)))
    back = contract(grad_rows, down, ((1,), (1,)))
    activation, slope = gelu_pair(hidden)
    v_up = contract((back * slope).astype(bf16), left, ((1,), (0,)))
    u_down = contract(activation.astype(bf16), right, ((1,), (0,)))
    return v_up, u_down


def all_units(senders, rows, near, late, fetches, results):
    weights, *groups = near
    right_up, left_down, *others = late
    (terms,) = results
    unpacked = unpack_weights(weights[...], senders, rows, lane)
    for fetch in fetches[:2]:
        fetch.wait()
    first, second = 0.0, 0.0
    for k, group in enumerate((*groups, *others)):
        if k >= len(groups):
            fetches[2 + k - len(groups)].wait()
        token_rows, grad_rows = group[0], group[1]
        v_up, u_down = through_units(token_rows, grad_rows, unpacked)
        u_up = contract(token_rows, right_up[...], ((1,), (0,))).astype(bf16)
        v_down = contract(grad_rows, left_down[...], ((1,), (0,))).astype(bf16)
        first += contract(v_up.astype(bf16), u_up, ((0,), (0,)))
        second += contract(v_down, u_down.astype(bf16), ((0,), (0,)))
    both = jnp.stack([first, second]).astype(bf16)
    terms[...] = jnp.broadcast_to(both[None], terms.shape)


def held(arrays, space):
    return [pltpu.with_memory_space_constraint(a, space) for a in arrays]


def kernel(body, results, near, late=(), flops=0):
    def run(*refs):
        at, parts = 0, []
        for size in (len(near), len(late), len(results), len(late)):
            parts.append(refs[at : at + size])
            at += size
        near_refs, sources, result_refs, late_refs = parts
        fetches = [
            pltpu.make_async_copy(source, target, refs[at].at[i])
            for i, (source, target) in enumerate(zip(sources, late_refs))
        ]
        for fetch in fetches:
            fetch.start()
        body(near_refs, late_refs, fetches, result_refs)

    spec = pl.BlockSpec(memory_space=pltpu.VMEM)
    scratch = [pltpu.VMEM(a.shape, a.dtype) for a in late]
    call = pl.pallas_call(
        run,
        out_shape=tuple(pltpu.HBM(shape, dtype) for shape, dtype in results),
        in_specs=[spec] * len(near) + [pl.BlockSpec(memory_space=pltpu.HBM)] * len(late),
        out_specs=(spec,) * len(results),
        scratch_shapes=scratch + [pltpu.SemaphoreType.DMA((max(1, len(late)),))],
        compiler_params=pltpu.CompilerParams(vmem_limit_bytes=kernel_vmem),
        cost_estimate=pl.CostEstimate(flops=flops, bytes_accessed=10**6, transcendentals=0),
    )
    return call(*held(near, pltpu.VMEM), *held(late, pltpu.HBM))


def neighbour(array, shift):
    return lax.ppermute(array, "x", [(i, (i + shift) % 4) for i in range(4)])


def pad_rows(tokens):
    count, width = tokens.shape[-2:]
    return jnp.pad(tokens.reshape(count, width), ((0, -count % 8), (0, 0)))


def local(
    images, out_grads, up_weight_t, down_weight_t, left_up, right_up, left_down, right_down, noise
):
    tokens = images.shape[2]
    rank = right_up.shape[1]
    senders = lax.axis_size(DP)
    shards = (up_weight_t, down_weight_t, left_up, right_down)
    rows = up_weight_t.shape[0]
    blocks = -(-rows * sum(shard.shape[1] for shard in shards) // (8 * lane))
    size = (senders, blocks * 8, lane)
    (copies,) = kernel(pack_weights, [(size, bf16)], (), shards)
    gathered = lax.all_to_all(copies, DP, 0, 0, tiled=True)
    gathered = gathered.reshape(senders, blocks, 8, lane).transpose(0, 2, 1, 3)
    gathered = gathered.reshape(senders * 8, blocks * lane)
    mine = jnp.stack([pad_rows(images), pad_rows(out_grads)])
    far = neighbour(mine, 2)
    below, above = (neighbour(mine, shift) for shift in (1, -1))
    swapped = []
    for group in (mine, far, below, above):
        swapped.append(lax.ppermute(group, "core", [(0, 1), (1, 0)]))
    all_augs = lax.axis_size(AUG)
    units = functools.partial(all_units, senders, rows)
    size = (all_augs, 2, rank, rank)
    near = (gathered, mine, below, above)
    late = (right_up, left_down, far, *swapped)
    (terms,) = kernel(units, [(size, bf16)], near, late, flops=4 * 10**9)
    share_rows = rank // all_augs
    lower_row = lax.axis_index(AUG) * share_rows
    aug_mean = lax.all_to_all(terms, AUG, 0, 0, tiled=True).astype(f32).sum(axis=0) / all_augs
    squares = jnp.sum(aug_mean * aug_mean)
    my_rows = lax.dynamic_slice_in_dim(aug_mean, lower_row, share_rows, 1)
    norm = jnp.sqrt(squares + 1e-06)
    clip_norm = clip_frac * rank * math.sqrt(tokens / all_augs)
    clip_scale = jnp.minimum(1.0, clip_norm / norm)
    summed_rows = of_everyone(of_everyone(clip_scale * my_rows, "dp_0"), "dp_1")
    all_images = lax.axis_size(DP)
    update = (summed_rows + noise_mult * clip_norm * noise) / jnp.sqrt(jnp.float32(all_images))
    return (update, clip_scale.reshape(1))


def solution(mesh):
    torus = Mesh(mesh.devices.reshape(8, 8, 4, 2), ("dp_0", "dp_1", "x", "core"))
    everyone = ("dp_0", "dp_1", "x", "core")
    placed = (
        P(AUG, DP, None, None),
        P(AUG, DP, None, None),
        P(everyone, None),
        P(everyone, None),
        P(everyone, None),
        P(),
        P(),
        P(everyone, None),
        P(None, AUG, None),
    )
    return jax.shard_map(
        local, mesh=torus, in_specs=placed, out_specs=(P(None, AUG, None), P(DP)), check_vma=False
    )
```

```python
import functools
import math

import jax
import jax.numpy as jnp
from jax import lax
from jax.experimental import pallas as pl
from jax.experimental.pallas import tpu as pltpu
from jax.sharding import Mesh
from jax.sharding import PartitionSpec as P


DP = ("dp_0", "dp_1")
AUG = ("x", "core")
bf16 = jnp.bfloat16
f32 = jnp.float32


gelu_coef = 0.7978845608028654
clip_frac = 0.3
noise_mult = 0.05
kernel_vmem = 24 * 2**20
lane = 128


def copy_for_each(shard, axis):
    size = lax.axis_size(axis)
    return lax.all_to_all(
        jnp.broadcast_to(shard[None], (size, *shard.shape)), axis, 0, 0, tiled=True
    )


def of_everyone(shard, axis):
    return copy_for_each(shard, axis).astype(f32).sum(axis=0)


def gelu_pair(hidden):
    square = hidden * hidden
    inner = hidden * (gelu_coef + (gelu_coef * 0.044715) * square)
    upper = 0.5 + 0.5 * jnp.tanh(inner)
    value = hidden * upper
    bend = 2.0 * gelu_coef + (6.0 * 0.044715 * gelu_coef) * square
    slope = upper + value * (1.0 - upper) * bend
    return (value, slope)


def contract(left, right, dims):
    return lax.dot_general(left, right, ((dims[0], dims[1]), ((), ())), preferred_element_type=f32)


def pack_weights(_, shards, fetches, results):
    (copies,) = results
    count, height, _ = copies.shape
    for fetch in fetches:
        fetch.wait()
    columns = [
        shard[:, at : at + lane].astype(f32)
        for shard in shards
        for at in range(0, shard.shape[1], lane)
    ]
    spare = height - sum(column.shape[0] for column in columns)
    columns.append(jnp.zeros((spare, lane), f32))
    tall = jnp.concatenate(columns, axis=0).astype(bf16)
    copies[...] = jnp.broadcast_to(tall[None], (count, height, lane))


def unpack_weights(gathered, senders, rows, lane):
    height, wide = gathered.shape
    tile, block = height // senders, min(senders, 32)
    columns = wide // lane * tile // rows
    size = block * tile
    at = lax.broadcasted_iota(jnp.int32, (size, size), 0)
    of = lax.broadcasted_iota(jnp.int32, (size, size), 1)
    select = (of == (at % block) * tile + at // block).astype(f32).astype(bf16)
    parts = []
    for first in range(0, height, size):
        both = contract(select, gathered[first : first + size], ((1,), (0,))).astype(bf16)

        def cell(row, column):
            t, s = divmod(column * rows + row, tile)
            return both[s * block : (s + 1) * block, t * lane : (t + 1) * lane]

        for row in range(rows):
            parts.append([cell(row, column) for column in range(columns)])
    half = (columns - 2) // 2
    wides = [
        jnp.concatenate([jnp.concatenate(p[lo : lo + half], axis=1) for p in parts], axis=0)
        for lo in (0, half)
    ]
    narrows = [jnp.concatenate([p[c] for p in parts], axis=0) for c in (columns - 2, columns - 1)]
    return (*wides, *narrows)


def through_units(token_rows, grad_rows, weights):
    up, down, left, right = weights
    hidden = contract(token_rows, up, ((1,), (1,)))
    back = contract(grad_rows, down, ((1,), (1,)))
    activation, slope = gelu_pair(hidden)
    v_up = contract((back * slope).astype(bf16), left, ((1,), (0,)))
    u_down = contract(activation.astype(bf16), right, ((1,), (0,)))
    return v_up, u_down


def all_units(senders, rows, near, late, fetches, results):
    weights, *groups = near
    right_up, left_down, *others = late
    (terms,) = results
    unpacked = unpack_weights(weights[...], senders, rows, lane)
    for fetch in fetches[:2]:
        fetch.wait()
    first, second = 0.0, 0.0
    for batch in (groups + others[:1], others[1:]):
        for fetch in fetches[2:3] if batch[0] is groups[0] else fetches[3:]:
            fetch.wait()
        token_rows = jnp.concatenate([group[0] for group in batch], axis=0)
        grad_rows = jnp.concatenate([group[1] for group in batch], axis=0)
        v_up, u_down = through_units(token_rows, grad_rows, unpacked)
        u_up = contract(token_rows, right_up[...], ((1,), (0,))).astype(bf16)
        v_down = contract(grad_rows, left_down[...], ((1,), (0,))).astype(bf16)
        first += contract(v_up.astype(bf16), u_up, ((0,), (0,)))
        second += contract(v_down, u_down.astype(bf16), ((0,), (0,)))
    both = jnp.stack([first, second]).astype(bf16)
    terms[...] = jnp.broadcast_to(both[None], terms.shape)


def held(arrays, space):
    return [pltpu.with_memory_space_constraint(a, space) for a in arrays]


def kernel(body, results, near, late=(), flops=0):
    def run(*refs):
        at, parts = 0, []
        for size in (len(near), len(late), len(results), len(late)):
            parts.append(refs[at : at + size])
            at += size
        near_refs, sources, result_refs, late_refs = parts
        fetches = [
            pltpu.make_async_copy(source, target, refs[at].at[i])
            for i, (source, target) in enumerate(zip(sources, late_refs))
        ]
        for fetch in fetches:
            fetch.start()
        body(near_refs, late_refs, fetches, result_refs)

    spec = pl.BlockSpec(memory_space=pltpu.VMEM)
    scratch = [pltpu.VMEM(a.shape, a.dtype) for a in late]
    call = pl.pallas_call(
        run,
        out_shape=tuple(pltpu.HBM(shape, dtype) for shape, dtype in results),
        in_specs=[spec] * len(near) + [pl.BlockSpec(memory_space=pltpu.HBM)] * len(late),
        out_specs=(spec,) * len(results),
        scratch_shapes=scratch + [pltpu.SemaphoreType.DMA((max(1, len(late)),))],
        compiler_params=pltpu.CompilerParams(vmem_limit_bytes=kernel_vmem),
        cost_estimate=pl.CostEstimate(flops=flops, bytes_accessed=10**6, transcendentals=0),
    )
    return call(*held(near, pltpu.VMEM), *held(late, pltpu.HBM))


def neighbour(array, shift):
    return lax.ppermute(array, "x", [(i, (i + shift) % 4) for i in range(4)])


def pad_rows(tokens):
    count, width = tokens.shape[-2:]
    return jnp.pad(tokens.reshape(count, width), ((0, -count % 8), (0, 0)))


def local(
    images, out_grads, up_weight_t, down_weight_t, left_up, right_up, left_down, right_down, noise
):
    tokens = images.shape[2]
    rank = right_up.shape[1]
    senders = lax.axis_size(DP)
    shards = (up_weight_t, down_weight_t, left_up, right_down)
    rows = up_weight_t.shape[0]
    blocks = -(-rows * sum(shard.shape[1] for shard in shards) // (8 * lane))
    size = (senders, blocks * 8, lane)
    (copies,) = kernel(pack_weights, [(size, bf16)], (), shards)
    gathered = lax.all_to_all(copies, DP, 0, 0, tiled=True)
    gathered = gathered.reshape(senders, blocks, 8, lane).transpose(0, 2, 1, 3)
    gathered = gathered.reshape(senders * 8, blocks * lane)
    mine = jnp.stack([pad_rows(images), pad_rows(out_grads)])
    far = neighbour(mine, 2)
    below, above = (neighbour(mine, shift) for shift in (1, -1))
    swapped = []
    for group in (mine, far, below, above):
        swapped.append(lax.ppermute(group, "core", [(0, 1), (1, 0)]))
    all_augs = lax.axis_size(AUG)
    units = functools.partial(all_units, senders, rows)
    size = (all_augs, 2, rank, rank)
    near = (gathered, mine, below, above)
    late = (right_up, left_down, far, *swapped)
    (terms,) = kernel(units, [(size, bf16)], near, late, flops=4 * 10**9)
    share_rows = rank // all_augs
    lower_row = lax.axis_index(AUG) * share_rows
    aug_mean = lax.all_to_all(terms, AUG, 0, 0, tiled=True).astype(f32).sum(axis=0) / all_augs
    squares = jnp.sum(aug_mean * aug_mean)
    my_rows = lax.dynamic_slice_in_dim(aug_mean, lower_row, share_rows, 1)
    norm = jnp.sqrt(squares + 1e-06)
    clip_norm = clip_frac * rank * math.sqrt(tokens / all_augs)
    clip_scale = jnp.minimum(1.0, clip_norm / norm)
    summed_rows = of_everyone(of_everyone(clip_scale * my_rows, "dp_0"), "dp_1")
    all_images = lax.axis_size(DP)
    update = (summed_rows + noise_mult * clip_norm * noise) / jnp.sqrt(jnp.float32(all_images))
    return (update, clip_scale.reshape(1))


def solution(mesh):
    torus = Mesh(mesh.devices.reshape(8, 8, 4, 2), ("dp_0", "dp_1", "x", "core"))
    everyone = ("dp_0", "dp_1", "x", "core")
    placed = (
        P(AUG, DP, None, None),
        P(AUG, DP, None, None),
        P(everyone, None),
        P(everyone, None),
        P(everyone, None),
        P(),
        P(),
        P(everyone, None),
        P(None, AUG, None),
    )
    return jax.shard_map(
        local, mesh=torus, in_specs=placed, out_specs=(P(None, AUG, None), P(DP)), check_vma=False
    )
```

```python
import functools
import math

import jax
import jax.numpy as jnp
from jax import lax
from jax.experimental import pallas as pl
from jax.experimental.pallas import tpu as pltpu
from jax.sharding import Mesh
from jax.sharding import PartitionSpec as P


DP = ("dp_0", "dp_1")
AUG = ("x", "core")
bf16 = jnp.bfloat16
f32 = jnp.float32


gelu_coef = 0.7978845608028654
clip_frac = 0.3
noise_mult = 0.05
kernel_vmem = 24 * 2**20
lane = 128


def copy_for_each(shard, axis):
    size = lax.axis_size(axis)
    return lax.all_to_all(
        jnp.broadcast_to(shard[None], (size, *shard.shape)), axis, 0, 0, tiled=True
    )


def of_everyone(shard, axis):
    return copy_for_each(shard, axis).astype(f32).sum(axis=0)


def gelu_pair(hidden):
    square = hidden * hidden
    inner = hidden * (gelu_coef + (gelu_coef * 0.044715) * square)
    upper = 0.5 + 0.5 * jnp.tanh(inner)
    value = hidden * upper
    bend = 2.0 * gelu_coef + (6.0 * 0.044715 * gelu_coef) * square
    slope = upper + value * (1.0 - upper) * bend
    return (value, slope)


def contract(left, right, dims):
    return lax.dot_general(left, right, ((dims[0], dims[1]), ((), ())), preferred_element_type=f32)


def pack_weights(_, shards, fetches, results):
    (copies,) = results
    count, height, _ = copies.shape
    for fetch in fetches:
        fetch.wait()
    columns = [
        shard[:, at : at + lane].astype(f32)
        for shard in shards
        for at in range(0, shard.shape[1], lane)
    ]
    spare = height - sum(column.shape[0] for column in columns)
    columns.append(jnp.zeros((spare, lane), f32))
    tall = jnp.concatenate(columns, axis=0).astype(bf16)
    copies[...] = jnp.broadcast_to(tall[None], (count, height, lane))


def unpack_weights(gathered, senders, rows, lane):
    height, wide = gathered.shape
    tile, block = height // senders, min(senders, 32)
    columns = wide // lane * tile // rows
    size = block * tile
    at = lax.broadcasted_iota(jnp.int32, (size, size), 0)
    of = lax.broadcasted_iota(jnp.int32, (size, size), 1)
    select = (of == (at % block) * tile + at // block).astype(f32).astype(bf16)
    parts = []
    for first in range(0, height, size):
        both = contract(select, gathered[first : first + size], ((1,), (0,))).astype(bf16)

        def cell(row, column):
            t, s = divmod(column * rows + row, tile)
            return both[s * block : (s + 1) * block, t * lane : (t + 1) * lane]

        for row in range(rows):
            parts.append([cell(row, column) for column in range(columns)])
    half = (columns - 2) // 2
    wides = [
        jnp.concatenate([jnp.concatenate(p[lo : lo + half], axis=1) for p in parts], axis=0)
        for lo in (0, half)
    ]
    narrows = [jnp.concatenate([p[c] for p in parts], axis=0) for c in (columns - 2, columns - 1)]
    return (*wides, *narrows)


def through_units(token_rows, grad_rows, weights):
    up, down, left, right = weights
    hidden = contract(token_rows, up, ((1,), (1,)))
    back = contract(grad_rows, down, ((1,), (1,)))
    activation, slope = gelu_pair(hidden)
    v_up = contract((back * slope).astype(bf16), left, ((1,), (0,)))
    u_down = contract(activation.astype(bf16), right, ((1,), (0,)))
    return v_up, u_down


def batches(groups, others, fetches):
    for batch, waits in ((groups + others[:1], fetches[:1]), (others[1:], fetches[1:])):
        for fetch in waits:
            fetch.wait()
        yield tuple(jnp.concatenate([group[i] for group in batch], axis=0) for i in (0, 1))


def project(near, late, fetches, results):
    right_up, left_down, *others = late
    for fetch in fetches[:2]:
        fetch.wait()
    for k, (token_rows, grad_rows) in enumerate(batches(list(near), others, fetches[2:])):
        results[0][k] = contract(token_rows, right_up[...], ((1,), (0,))).astype(bf16)
        results[1][k] = contract(grad_rows, left_down[...], ((1,), (0,))).astype(bf16)


def all_units(senders, rows, near, late, fetches, results):
    weights, *groups = near
    u_up, v_down, *others = late
    (terms,) = results
    unpacked = unpack_weights(weights[...], senders, rows, lane)
    for fetch in fetches[:2]:
        fetch.wait()
    first, second = 0.0, 0.0
    for k, (token_rows, grad_rows) in enumerate(batches(groups, others, fetches[2:])):
        v_up, u_down = through_units(token_rows, grad_rows, unpacked)
        first += contract(v_up.astype(bf16), u_up[k], ((0,), (0,)))
        second += contract(v_down[k], u_down.astype(bf16), ((0,), (0,)))
    both = jnp.stack([first, second]).astype(bf16)
    terms[...] = jnp.broadcast_to(both[None], terms.shape)


def held(arrays, space):
    return [pltpu.with_memory_space_constraint(a, space) for a in arrays]


def kernel(body, results, near, late=(), flops=0):
    def run(*refs):
        at, parts = 0, []
        for size in (len(near), len(late), len(results), len(late)):
            parts.append(refs[at : at + size])
            at += size
        near_refs, sources, result_refs, late_refs = parts
        fetches = [
            pltpu.make_async_copy(source, target, refs[at].at[i])
            for i, (source, target) in enumerate(zip(sources, late_refs))
        ]
        for fetch in fetches:
            fetch.start()
        body(near_refs, late_refs, fetches, result_refs)

    spec = pl.BlockSpec(memory_space=pltpu.VMEM)
    scratch = [pltpu.VMEM(a.shape, a.dtype) for a in late]
    call = pl.pallas_call(
        run,
        out_shape=tuple(pltpu.HBM(shape, dtype) for shape, dtype in results),
        in_specs=[spec] * len(near) + [pl.BlockSpec(memory_space=pltpu.HBM)] * len(late),
        out_specs=(spec,) * len(results),
        scratch_shapes=scratch + [pltpu.SemaphoreType.DMA((max(1, len(late)),))],
        compiler_params=pltpu.CompilerParams(vmem_limit_bytes=kernel_vmem),
        cost_estimate=pl.CostEstimate(flops=flops, bytes_accessed=10**6, transcendentals=0),
    )
    return call(*held(near, pltpu.VMEM), *held(late, pltpu.HBM))


def neighbour(array, shift):
    return lax.ppermute(array, "x", [(i, (i + shift) % 4) for i in range(4)])


def pad_rows(tokens):
    count, width = tokens.shape[-2:]
    return jnp.pad(tokens.reshape(count, width), ((0, -count % 8), (0, 0)))


def local(
    images, out_grads, up_weight_t, down_weight_t, left_up, right_up, left_down, right_down, noise
):
    tokens = images.shape[2]
    rank = right_up.shape[1]
    senders = lax.axis_size(DP)
    shards = (up_weight_t, down_weight_t, left_up, right_down)
    rows = up_weight_t.shape[0]
    blocks = -(-rows * sum(shard.shape[1] for shard in shards) // (8 * lane))
    size = (senders, blocks * 8, lane)
    (copies,) = kernel(pack_weights, [(size, bf16)], (), shards)
    gathered = lax.all_to_all(copies, DP, 0, 0, tiled=True)
    gathered = gathered.reshape(senders, blocks, 8, lane).transpose(0, 2, 1, 3)
    gathered = gathered.reshape(senders * 8, blocks * lane)
    mine = jnp.stack([pad_rows(images), pad_rows(out_grads)])
    far = neighbour(mine, 2)
    below, above = (neighbour(mine, shift) for shift in (1, -1))
    swapped = []
    for group in (mine, far, below, above):
        swapped.append(lax.ppermute(group, "core", [(0, 1), (1, 0)]))
    all_augs = lax.axis_size(AUG)
    units = functools.partial(all_units, senders, rows)
    size = (all_augs, 2, rank, rank)
    near, others = (mine, below, above), (far, *swapped)
    half = (2, (len(near) + len(others)) // 2 * mine.shape[1], rank)
    kept = kernel(project, [(half, bf16)] * 2, near, (right_up, left_down, *others), 10**9)
    (terms,) = kernel(units, [(size, bf16)], (gathered, *near), (*kept, *others), 4 * 10**9)
    share_rows = rank // all_augs
    lower_row = lax.axis_index(AUG) * share_rows
    aug_mean = lax.all_to_all(terms, AUG, 0, 0, tiled=True).astype(f32).sum(axis=0) / all_augs
    squares = jnp.sum(aug_mean * aug_mean)
    my_rows = lax.dynamic_slice_in_dim(aug_mean, lower_row, share_rows, 1)
    norm = jnp.sqrt(squares + 1e-06)
    clip_norm = clip_frac * rank * math.sqrt(tokens / all_augs)
    clip_scale = jnp.minimum(1.0, clip_norm / norm)
    summed_rows = of_everyone(of_everyone(clip_scale * my_rows, "dp_0"), "dp_1")
    all_images = lax.axis_size(DP)
    update = (summed_rows + noise_mult * clip_norm * noise) / jnp.sqrt(jnp.float32(all_images))
    return (update, clip_scale.reshape(1))


def solution(mesh):
    torus = Mesh(mesh.devices.reshape(8, 8, 4, 2), ("dp_0", "dp_1", "x", "core"))
    everyone = ("dp_0", "dp_1", "x", "core")
    placed = (
        P(AUG, DP, None, None),
        P(AUG, DP, None, None),
        P(everyone, None),
        P(everyone, None),
        P(everyone, None),
        P(),
        P(),
        P(everyone, None),
        P(None, AUG, None),
    )
    return jax.shard_map(
        local, mesh=torus, in_specs=placed, out_specs=(P(None, AUG, None), P(DP)), check_vma=False
    )
```
